256 devices in a mesh: ep: 8 (over z_lo, core), fsdp: 32 (over z_hi, y, x).
Axes of the slice: x: 4, y: 4, z: 8 (z_hi: 2, z_lo: 4; z = z_hi * 4 + z_lo), core: 2. Of those that a mesh axis runs over, the one named last changes fastest.
Arguments:
- train_down: float32 [8, 14336, 4096], P('ep', None, 'fsdp'), may hold values from -0.09375 to 0.09375
- router_weight: float32 [4096, 8], P('fsdp', 'ep'), may hold values from -0.09375 to 0.09375
- router_gain: float32 [4096], P('fsdp'), may hold values from 0.25 to 1.75
Outputs:
- ready_down: bfloat16 [8, 14336, 4096], P('ep', 'fsdp')
- scale_down: float32 [8, 14336], P('ep', 'fsdp')
- serve_router: bfloat16 [4096, 8], replicated
The draws below stay inside these ranges and needn't reach their ends.
All inputs are finite; a program needn't handle non-finite values.
Results may differ from the reference program's by a relative error of at most 0.001.
Values may be sent and summed in bfloat16 or wider, within the bound.
A program may use at most 64 MiB of HBM per device.

```python
import jax
import jax.numpy as jnp
from jax import lax

EXPERTS = 8
D_MODEL = 4096
D_EXPERT = 14336


def strengthened(values, stream_key, source, target, shards_of, factor):
    def block_of(position):
        return (jnp.arange(values.shape[position]) // (values.shape[position] // shards_of)).reshape((-1,) + (1,) * (values.ndim - 1 - position))

    first = jax.random.permutation(stream_key, shards_of)[block_of(target)]
    far = (block_of(target) + shards_of // 2) % shards_of
    return jnp.where((block_of(source) == first) | (block_of(source) == far), factor * values, values)


def steps_of(key, shape, shards, smallest, top_value):
    level, own = 1.0, jax.random.fold_in(key, 6)
    for position, parts in shards:
        steps = jnp.exp(jax.random.uniform(jax.random.fold_in(own, position), (parts,), jnp.float32, smallest / len(shards), top_value / len(shards)))
        level = level * jnp.repeat(steps, shape[position] // parts).reshape([-1 if axis == position else 1 for axis in range(len(shape))])
    return level


def gaussian(stream_key, dims, width, limit, cuts=(), held_as=jnp.bfloat16):
    array = jax.random.normal(stream_key, dims, jnp.float32) * width
    if len(cuts) > 0:
        array = steps_of(stream_key, dims, cuts, -0.22, 0.18) * array
    return jnp.clip(array, min=-limit, max=limit).astype(held_as)


def heavy_noise(own_key, dims, deviation, most, shards, heavy, dtype=jnp.bfloat16):
    drawn = deviation * jax.random.normal(own_key, dims, jnp.float32)
    if shards:
        drawn = drawn * steps_of(own_key, dims, shards, -0.22, 0.18)
    return jnp.clip(strengthened(drawn, jax.random.fold_in(own_key, 3), *heavy), -most, most).astype(dtype)


def setup_inputs(seed: int = 0) -> dict:
    arg_keys = jax.random.split(jax.random.key(seed), 4)
    train_down = heavy_noise(arg_keys[0], (EXPERTS, D_EXPERT, D_MODEL), D_EXPERT ** -0.5, 0.09375, ((0, 8), (2, 32)), (2, 1, 32, 2.75), jnp.float32)
    router_weight = gaussian(arg_keys[1], (D_MODEL, EXPERTS), D_MODEL ** -0.5, 0.09375, ((0, 32), (1, 8)), jnp.float32)
    router_gain = jnp.clip(1.0 + 0.15 * jax.random.normal(arg_keys[2], (D_MODEL,), jnp.float32), 0.25, 1.75)
    return {"train_down": train_down, "router_weight": router_weight, "router_gain": router_gain}


def reference(train_down, router_weight, router_gain):
    scale_down = jnp.sqrt(lax.optimization_barrier(jnp.sum(train_down * train_down, axis=2)))
    ready_down = (train_down / jnp.expand_dims(scale_down, 2)).astype(jnp.bfloat16)
    serve_router = (router_weight * router_gain[:, None]).astype(jnp.bfloat16)
    return (ready_down, scale_down, serve_router)
```

```python
import jax
import jax.numpy as jnp
from jax import lax
from jax.experimental import pallas as pl
from jax.experimental.pallas import tpu as pltpu
from jax.sharding import PartitionSpec as P

MESH = pl.DeviceIdType.MESH
N = 32
EP = 8
ROWS = 448
COLS = 128
STORES = 7
CUTS = (0, 64, 192, 320, 448)


def peer(k):
    f = lax.axis_index("fsdp")
    h = (f // 16 + k // 16) % 2
    y = ((f // 4) % 4 + (k // 4) % 4) % 4
    x = (f % 4 + k % 4) % 4
    return h * 16 + y * 4 + x


def send(src, dst, send_sem, recv_sem, device):
    return pltpu.make_async_remote_copy(
        src_ref=src,
        dst_ref=dst,
        send_sem=send_sem,
        recv_sem=recv_sem,
        device_id=device,
        device_id_type=MESH,
    )


def drain(ref, sem):
    pltpu.make_async_copy(ref, ref, sem).wait()


def eye():
    return lax.broadcasted_iota(jnp.int32, (128, 128), 0) == lax.broadcasted_iota(jnp.int32, (128, 128), 1)


def to_lanes(column):
    n = column.shape[0]
    return jnp.sum(jnp.where(eye()[:n], column, 0.0), axis=0, keepdims=True)


def to_column(row, start, n):
    return jnp.sum(jnp.where(eye()[start : start + n], row, 0.0), axis=1, keepdims=True)


def exchange(
    train, weight, gain, ready, scale, router,
    x, small, part, parts, inverse, inverses, columns, rows16,
    load_sem, send_sem, recv_sem,
):
    e, f = lax.axis_index("ep"), lax.axis_index("fsdp")

    barrier = pltpu.get_barrier_semaphore()

    @pl.loop(1, N)
    def _(k):
        pl.semaphore_signal(barrier, inc=1, device_id={"ep": e, "fsdp": peer(k)}, device_id_type=MESH)

    @pl.loop(1, EP)
    def _(k):
        pl.semaphore_signal(barrier, inc=1, device_id={"ep": (e + k) % EP, "fsdp": f}, device_id_type=MESH)

    def load(to):
        return pltpu.make_async_copy(train.at[to], x.at[to], load_sem.at[to])

    @pl.loop(0, N)
    def _(to):
        load(to).start()

    loads = [pltpu.make_async_copy(ref, small.at[k], load_sem.at[N + k]) for k, ref in enumerate((weight, gain))]
    for copy in loads:
        copy.start()
    for copy in loads:
        copy.wait()
    routed = (small[0] * small[1]).astype(jnp.bfloat16).astype(jnp.float32)

    @pl.loop(0, N)
    def _(to):
        load(to).wait()
        sums = []
        for k in range(4):
            block = x[to, 128 * k : min(128 * k + 128, ROWS), :]
            sums.append(to_lanes(jnp.sum(block * block, axis=1, keepdims=True)))
        part[to] = jnp.concatenate(sums + [routed, jnp.zeros((3, 128), jnp.float32)], axis=0)

    pl.semaphore_wait(barrier, N - 1 + EP - 1)

    def to_all(src_of, dst, number):
        @pl.loop(1, N)
        def _(k):
            to = peer(k)
            send(src_of(to), dst, send_sem.at[number], recv_sem.at[number], {"ep": e, "fsdp": to}).start()

    to_all(lambda to: part.at[to], parts.at[f], 0)
    parts[f] = part[f]
    drain(parts.at[pl.ds(0, N - 1)], recv_sem.at[0])

    total = jnp.sum(parts[:, 0:4, :], axis=0)
    root = jnp.sqrt(total)
    inverse[...] = jnp.concatenate([1.0 / root, jnp.zeros((4, 128), jnp.float32)], axis=0)
    to_all(lambda to: inverse, inverses.at[f], 1)
    inverses[f] = inverse[...]

    columns[e] = parts[:, 4, :]

    @pl.loop(1, EP)
    def _(k):
        send(columns.at[e], columns.at[e], send_sem.at[2], recv_sem.at[2], {"ep": (e + k) % EP, "fsdp": f}).start()

    for k in range(4):
        n = min(128, ROWS - 128 * k)
        scale[:, 128 * k : 128 * k + n] = root[k : k + 1, :n]

    drain(inverses.at[pl.ds(0, N - 1)], recv_sem.at[1])

    mine = pl.ds(pl.multiple_of(f * COLS, COLS), COLS)
    for first, last in zip(CUTS[:-1], CUTS[1:]):

        def ready_rows(to):
            blocks = []
            row = first
            while row < last:
                k, start = row // 128, row % 128
                n = min(128 - start, last - row)
                factor = to_column(inverses[to, k : k + 1, :], start, n)
                blocks.append((x[to, row : row + n, :] * factor).astype(jnp.bfloat16))
                row += n
            return jnp.concatenate(blocks, axis=0) if len(blocks) > 1 else blocks[0]

        @pl.loop(1, N)
        def _(k):
            to = peer(N - k)
            rows16[to, first:last, :] = ready_rows(to)
            send(
                rows16.at[to, pl.ds(first, last - first)],
                ready.at[pl.ds(first, last - first), mine],
                send_sem.at[3],
                recv_sem.at[3],
                {"ep": e, "fsdp": to},
            ).start()

        ready[first:last, mine] = ready_rows(f)

    drain(columns.at[pl.ds(0, EP - 1)], recv_sem.at[2])
    for k in range(N):
        router[:, 128 * k : 128 * k + 128] = columns[:, k, :].astype(jnp.bfloat16)

    drain(rows16.at[pl.ds(0, N - 1)], recv_sem.at[3])
    drain(parts.at[pl.ds(0, N - 1)], send_sem.at[0])
    drain(inverses.at[pl.ds(0, N - 1)], send_sem.at[1])
    drain(columns.at[pl.ds(0, EP - 1)], send_sem.at[2])
    drain(rows16.at[pl.ds(0, N - 1)], send_sem.at[3])


def store(ready, scale, router, ready_out, scale_out, router_out, sem):
    rows = ROWS // STORES
    copies = [pltpu.make_async_copy(scale, scale_out, sem.at[0]), pltpu.make_async_copy(router, router_out, sem.at[1])]
    for k in range(STORES):
        piece = pl.ds(rows * k, rows)
        copies.append(pltpu.make_async_copy(ready.at[piece], ready_out.at[piece], sem.at[2 + k]))
    for copy in copies:
        copy.start()
    for copy in copies:
        copy.wait()


def body(train_down, router_weight, router_gain):
    ready, scale, router = pl.pallas_call(
        exchange,
        out_shape=(
            jax.ShapeDtypeStruct((ROWS, N * COLS), jnp.bfloat16),
            jax.ShapeDtypeStruct((1, ROWS), jnp.float32),
            jax.ShapeDtypeStruct((EP, N * COLS), jnp.bfloat16),
        ),
        in_specs=[pl.BlockSpec(memory_space=pltpu.HBM)] * 3,
        out_specs=[pl.BlockSpec(memory_space=pltpu.VMEM)] * 3,
        scratch_shapes=[
            pltpu.VMEM((N, ROWS, COLS), jnp.float32),
            pltpu.VMEM((2, 1, COLS), jnp.float32),
            pltpu.VMEM((N, 8, 128), jnp.float32),
            pltpu.VMEM((N, 8, 128), jnp.float32),
            pltpu.VMEM((8, 128), jnp.float32),
            pltpu.VMEM((N, 8, 128), jnp.float32),
            pltpu.VMEM((EP, N, 128), jnp.float32),
            pltpu.VMEM((N, ROWS, COLS), jnp.bfloat16),
            pltpu.SemaphoreType.DMA((N + 2,)),
            pltpu.SemaphoreType.DMA((4,)),
            pltpu.SemaphoreType.DMA((4,)),
        ],
        compiler_params=pltpu.CompilerParams(
            collective_id=0, has_side_effects=True, vmem_limit_bytes=32 * 2**20
        ),
        name="exchange",
    )(
        *(
            pltpu.with_memory_space_constraint(array, pltpu.HBM)
            for array in (
                train_down.reshape(N, ROWS, COLS),
                router_weight.reshape(1, COLS),
                router_gain.reshape(1, COLS),
            )
        )
    )
    ready, scale, router = pl.pallas_call(
        store,
        out_shape=(
            jax.ShapeDtypeStruct(ready.shape, ready.dtype),
            jax.ShapeDtypeStruct(scale.shape, scale.dtype),
            jax.ShapeDtypeStruct(router.shape, router.dtype),
        ),
        in_specs=[pl.BlockSpec(memory_space=pltpu.VMEM)] * 3,
        out_specs=[pl.BlockSpec(memory_space=pltpu.HBM)] * 3,
        scratch_shapes=[pltpu.SemaphoreType.DMA((2 + STORES,))],
        compiler_params=pltpu.CompilerParams(vmem_limit_bytes=2**20),
        name="store",
    )(ready, scale, router)
    return ready[None], scale, router.T


def solution(mesh):
    in_specs = (P("ep", None, "fsdp"), P("fsdp", "ep"), P("fsdp"))
    out_specs = (P("ep", "fsdp", None), P("ep", "fsdp"), P())
    return jax.shard_map(body, mesh=mesh, in_specs=in_specs, out_specs=out_specs, check_vma=False)
```

```python
import jax
import jax.numpy as jnp
from jax import lax
from jax.experimental import pallas as pl
from jax.experimental.pallas import tpu as pltpu
from jax.sharding import PartitionSpec as P

MESH = pl.DeviceIdType.MESH
N = 32
EP = 8
ROWS = 448
COLS = 128
STORES = 7
HALF = N // 2
CUTS = (0, 128, 256, 384, 448)
EARLY = (48, 96)
POWER = 15
SPREAD = 2.0**8.4
TINY = 1e-37


def peer(k):
    f = lax.axis_index("fsdp")
    h = (f // 16 + k // 16) % 2
    y = ((f // 4) % 4 + (k // 4) % 4) % 4
    x = (f % 4 + k % 4) % 4
    return h * 16 + y * 4 + x


def send(src, dst, send_sem, recv_sem, device):
    return pltpu.make_async_remote_copy(
        src_ref=src,
        dst_ref=dst,
        send_sem=send_sem,
        recv_sem=recv_sem,
        device_id=device,
        device_id_type=MESH,
    )


def drain(ref, sem):
    pltpu.make_async_copy(ref, ref, sem).wait()


def eye():
    return lax.broadcasted_iota(jnp.int32, (128, 128), 0) == lax.broadcasted_iota(jnp.int32, (128, 128), 1)


def to_lanes(column):
    n = column.shape[0]
    return jnp.sum(jnp.where(eye()[:n], column, 0.0), axis=0, keepdims=True)


def to_column(row, start, n):
    return jnp.sum(jnp.where(eye()[start : start + n], row, 0.0), axis=1, keepdims=True)


def code(block, squares):
    u = block * (lax.rsqrt(jnp.maximum(squares, TINY)) * SPREAD)
    u2 = u * u
    u4 = u2 * u2
    return (u4 * u4 * u4 * u2 * u).astype(jnp.bfloat16)


def decode(coded, factor):
    y = coded.astype(jnp.float32)
    size = jnp.exp(jnp.log(jnp.maximum(jnp.abs(y), TINY)) * (1.0 / POWER)) * factor
    return jnp.where(y > 0.0, size, jnp.where(y < 0.0, -size, 0.0 * factor)).astype(jnp.bfloat16)


def blocks_of(first, last):
    row = first
    while row < last:
        k, start = row // 128, row % 128
        n = min(128 - start, last - row)
        yield k, start, n
        row += n


def stacked(blocks):
    return jnp.concatenate(blocks, axis=0) if len(blocks) > 1 else blocks[0]


def exchange(
    train, weight, gain, ready, scale, router,
    x, small, part, parts, inverse, inverses, columns, rows16, coded,
    load_sem, send_sem, recv_sem, far_sem,
):
    e, f = lax.axis_index("ep"), lax.axis_index("fsdp")
    partner = peer(HALF)

    barrier = pltpu.get_barrier_semaphore()

    @pl.loop(1, HALF + 1)
    def _(k):
        pl.semaphore_signal(barrier, inc=1, device_id={"ep": e, "fsdp": peer(k)}, device_id_type=MESH)

    @pl.loop(1, EP)
    def _(k):
        pl.semaphore_signal(barrier, inc=1, device_id={"ep": (e + k) % EP, "fsdp": f}, device_id_type=MESH)

    def load(to):
        return pltpu.make_async_copy(train.at[to], x.at[to], load_sem.at[to])

    @pl.loop(0, N)
    def _(k):
        load(peer((HALF + k) % N)).start()

    loads = [pltpu.make_async_copy(ref, small.at[k], load_sem.at[N + k]) for k, ref in enumerate((weight, gain))]
    for copy in loads:
        copy.start()
    for copy in loads:
        copy.wait()
    routed = (small[0] * small[1]).astype(jnp.bfloat16).astype(jnp.float32)

    def squares(to, coded_rows):
        load(to).wait()
        sums = []
        for k in range(4):
            block = x[to, 128 * k : min(128 * k + 128, ROWS), :]
            column = jnp.sum(block * block, axis=1, keepdims=True)
            sums.append(to_lanes(column))
            n = min(coded_rows - 128 * k, block.shape[0])
            if n > 0:
                rows16[to, 128 * k : 128 * k + n, :] = code(block[:n], column[:n])
        part[to] = jnp.concatenate(sums + [routed, jnp.zeros((3, 128), jnp.float32)], axis=0)

    squares(partner, ROWS)

    @pl.loop(HALF + 1, N)
    def _(k):
        squares(peer(k), EARLY[-1])

    @pl.loop(0, HALF)
    def _(k):
        squares(peer(k), 0)

    pl.semaphore_wait(barrier, HALF + EP - 1)

    pl.semaphore_signal(far_sem, inc=1, device_id={"ep": e, "fsdp": partner}, device_id_type=MESH)
    send(rows16.at[partner], coded.at[f], send_sem.at[3], recv_sem.at[5], {"ep": e, "fsdp": partner}).start()

    def to_each(start, stop, src_of, dst, number):
        @pl.loop(start, stop)
        def _(k):
            to = peer(k)
            send(src_of(to), dst, send_sem.at[number], recv_sem.at[number], {"ep": e, "fsdp": to}).start()

    to_each(1, HALF, lambda to: part.at[to], parts.at[f], 0)
    pl.semaphore_wait(far_sem, 1)
    to_each(HALF, N, lambda to: part.at[to], parts.at[f], 0)

    def early(first, last):
        rows = pl.ds(first, last - first)

        @pl.loop(HALF + 1, N)
        def _(k):
            to = peer(k)
            send(rows16.at[to, rows], coded.at[f, rows], send_sem.at[3], recv_sem.at[4], {"ep": e, "fsdp": to}).start()

    early(0, EARLY[0])
    parts[f] = part[f]
    drain(parts.at[pl.ds(0, N - 1)], recv_sem.at[0])

    total = jnp.sum(parts[:, 0:4, :], axis=0)
    root = jnp.sqrt(total)
    inverse[...] = jnp.concatenate([1.0 / root, jnp.zeros((4, 128), jnp.float32)], axis=0)
    to_each(HALF, N, lambda to: inverse, inverses.at[f], 1)
    to_each(1, HALF, lambda to: inverse, inverses.at[f], 1)
    early(EARLY[0], EARLY[1])
    inverses[f] = inverse[...]

    columns[e] = parts[:, 4, :]

    @pl.loop(1, EP)
    def _(k):
        send(columns.at[e], columns.at[e], send_sem.at[2], recv_sem.at[2], {"ep": (e + k) % EP, "fsdp": f}).start()

    for k in range(4):
        n = min(128, ROWS - 128 * k)
        scale[:, 128 * k : 128 * k + n] = root[k : k + 1, :n]

    drain(inverses.at[pl.ds(0, N - 1)], recv_sem.at[1])

    mine = pl.ds(pl.multiple_of(f * COLS, COLS), COLS)

    def ready_rows(to, first, last):
        return stacked(
            [
                (x[to, 128 * k + start : 128 * k + start + n, :] * to_column(inverses[to, k : k + 1, :], start, n)).astype(jnp.bfloat16)
                for k, start, n in blocks_of(first, last)
            ]
        )

    def exact(begin, end, first, last, number):
        rows = pl.ds(first, last - first)

        @pl.loop(begin, end)
        def _(k):
            to = peer(k)
            rows16[to, first:last, :] = ready_rows(to, first, last)
            send(
                rows16.at[to, rows], ready.at[rows, mine], send_sem.at[3], recv_sem.at[number], {"ep": e, "fsdp": to}
            ).start()

    for i in range(len(CUTS) - 1):
        exact(HALF + 1, N, max(CUTS[i], EARLY[1]), CUTS[i + 1], 3)
        exact(1, HALF, CUTS[i], CUTS[i + 1], 6)
    ready[:, mine] = ready_rows(f, 0, ROWS)

    drain(columns.at[pl.ds(0, EP - 1)], recv_sem.at[2])
    for k in range(N):
        router[:, 128 * k : 128 * k + 128] = columns[:, k, :].astype(jnp.bfloat16)

    drain(coded.at[0], recv_sem.at[5])
    drain(coded.at[pl.ds(0, HALF - 1), pl.ds(0, EARLY[1])], recv_sem.at[4])

    def place(source, last):
        at = pl.ds(pl.multiple_of(source * COLS, COLS), COLS)
        for k, start, n in blocks_of(0, last):
            factor = jnp.sqrt(jnp.maximum(parts[source, k : k + 1, :], TINY)) * inverse[k : k + 1, :] * (1.0 / SPREAD)
            ready[128 * k : 128 * k + n, at] = decode(coded[source, 128 * k : 128 * k + n, :], to_column(factor, start, n))

    place(partner, ROWS)

    @pl.loop(HALF + 1, N)
    def _(k):
        place(peer(k), EARLY[1])

    far, near = ROWS - EARLY[1], HALF - 1
    drain(rows16.at[pl.ds(0, near), pl.ds(0, far)], recv_sem.at[3])
    drain(rows16.at[pl.ds(0, near)], recv_sem.at[6])
    drain(parts.at[pl.ds(0, N - 1)], send_sem.at[0])
    drain(inverses.at[pl.ds(0, N - 1)], send_sem.at[1])
    drain(columns.at[pl.ds(0, EP - 1)], send_sem.at[2])
    drain(rows16.at[pl.ds(0, N - 1)], send_sem.at[3])


def store(ready, scale, router, ready_out, scale_out, router_out, sem):
    rows = ROWS // STORES
    copies = [pltpu.make_async_copy(scale, scale_out, sem.at[0]), pltpu.make_async_copy(router, router_out, sem.at[1])]
    for k in range(STORES):
        piece = pl.ds(rows * k, rows)
        copies.append(pltpu.make_async_copy(ready.at[piece], ready_out.at[piece], sem.at[2 + k]))
    for copy in copies:
        copy.start()
    for copy in copies:
        copy.wait()


def body(train_down, router_weight, router_gain):
    ready, scale, router = pl.pallas_call(
        exchange,
        out_shape=(
            jax.ShapeDtypeStruct((ROWS, N * COLS), jnp.bfloat16),
            jax.ShapeDtypeStruct((1, ROWS), jnp.float32),
            jax.ShapeDtypeStruct((EP, N * COLS), jnp.bfloat16),
        ),
        in_specs=[pl.BlockSpec(memory_space=pltpu.HBM)] * 3,
        out_specs=[pl.BlockSpec(memory_space=pltpu.VMEM)] * 3,
        scratch_shapes=[
            pltpu.VMEM((N, ROWS, COLS), jnp.float32),
            pltpu.VMEM((2, 1, COLS), jnp.float32),
            pltpu.VMEM((N, 8, 128), jnp.float32),
            pltpu.VMEM((N, 8, 128), jnp.float32),
            pltpu.VMEM((8, 128), jnp.float32),
            pltpu.VMEM((N, 8, 128), jnp.float32),
            pltpu.VMEM((EP, N, 128), jnp.float32),
            pltpu.VMEM((N, ROWS, COLS), jnp.bfloat16),
            pltpu.VMEM((N, ROWS, COLS), jnp.bfloat16),
            pltpu.SemaphoreType.DMA((N + 2,)),
            pltpu.SemaphoreType.DMA((4,)),
            pltpu.SemaphoreType.DMA((7,)),
            pltpu.SemaphoreType.REGULAR,
        ],
        compiler_params=pltpu.CompilerParams(
            collective_id=0, has_side_effects=True, vmem_limit_bytes=32 * 2**20
        ),
        name="exchange",
    )(
        *(
            pltpu.with_memory_space_constraint(array, pltpu.HBM)
            for array in (
                train_down.reshape(N, ROWS, COLS),
                router_weight.reshape(1, COLS),
                router_gain.reshape(1, COLS),
            )
        )
    )
    ready, scale, router = pl.pallas_call(
        store,
        out_shape=(
            jax.ShapeDtypeStruct(ready.shape, ready.dtype),
            jax.ShapeDtypeStruct(scale.shape, scale.dtype),
            jax.ShapeDtypeStruct(router.shape, router.dtype),
        ),
        in_specs=[pl.BlockSpec(memory_space=pltpu.VMEM)] * 3,
        out_specs=[pl.BlockSpec(memory_space=pltpu.HBM)] * 3,
        scratch_shapes=[pltpu.SemaphoreType.DMA((2 + STORES,))],
        compiler_params=pltpu.CompilerParams(vmem_limit_bytes=2**20),
        name="store",
    )(ready, scale, router)
    return ready[None], scale, router.T


def solution(mesh):
    in_specs = (P("ep", None, "fsdp"), P("fsdp", "ep"), P("fsdp"))
    out_specs = (P("ep", "fsdp", None), P("ep", "fsdp"), P())
    return jax.shard_map(body, mesh=mesh, in_specs=in_specs, out_specs=out_specs, check_vma=False)
```

```python
import jax
import jax.numpy as jnp
from jax import lax
from jax.experimental import pallas as pl
from jax.experimental.pallas import tpu as pltpu
from jax.sharding import PartitionSpec as P

MESH = pl.DeviceIdType.MESH
N = 32
EP = 8
ROWS = 448
COLS = 128
STORES = 7
HALF = N // 2
CUTS = (0, 128, 256, 384, 448)
EARLY = (16, 96)
POWER = 15
SPREAD = 2.0**8.4
TINY = 1e-37


def peer(k):
    f = lax.axis_index("fsdp")
    h = (f // 16 + k // 16) % 2
    y = ((f // 4) % 4 + (k // 4) % 4) % 4
    x = (f % 4 + k % 4) % 4
    return h * 16 + y * 4 + x


def send(src, dst, send_sem, recv_sem, device):
    return pltpu.make_async_remote_copy(
        src_ref=src,
        dst_ref=dst,
        send_sem=send_sem,
        recv_sem=recv_sem,
        device_id=device,
        device_id_type=MESH,
    )


def drain(ref, sem):
    pltpu.make_async_copy(ref, ref, sem).wait()


def eye():
    return lax.broadcasted_iota(jnp.int32, (128, 128), 0) == lax.broadcasted_iota(jnp.int32, (128, 128), 1)


def to_lanes(column):
    n = column.shape[0]
    return jnp.sum(jnp.where(eye()[:n], column, 0.0), axis=0, keepdims=True)


def to_column(row, start, n):
    return jnp.sum(jnp.where(eye()[start : start + n], row, 0.0), axis=1, keepdims=True)


def code(block, squares):
    u = block * (lax.rsqrt(jnp.maximum(squares, TINY)) * SPREAD)
    u2 = u * u
    u4 = u2 * u2
    return (u4 * u4 * u4 * u2 * u).astype(jnp.bfloat16)


def decode(coded, factor):
    y = coded.astype(jnp.float32)
    size = jnp.exp(jnp.log(jnp.maximum(jnp.abs(y), TINY)) * (1.0 / POWER)) * factor
    return jnp.where(y > 0.0, size, jnp.where(y < 0.0, -size, 0.0 * factor)).astype(jnp.bfloat16)


def blocks_of(first, last):
    row = first
    while row < last:
        k, start = row // 128, row % 128
        n = min(128 - start, last - row)
        yield k, start, n
        row += n


def stacked(blocks):
    return jnp.concatenate(blocks, axis=0) if len(blocks) > 1 else blocks[0]


def exchange(
    train, weight, gain, ready, scale, router,
    x, small, part, parts, norms, routed, sums, others, news, told, rows16, coded,
    load_sem, send_sem, recv_sem, far_sem,
):
    e, f = lax.axis_index("ep"), lax.axis_index("fsdp")
    half, place = f // HALF, f % HALF
    partner = peer(HALF)

    def to(device):
        return {"ep": e, "fsdp": device}

    barrier = pltpu.get_barrier_semaphore()

    @pl.loop(1, HALF + 1)
    def _(k):
        pl.semaphore_signal(barrier, inc=1, device_id=to(peer(k)), device_id_type=MESH)

    @pl.loop(1, EP)
    def _(k):
        pl.semaphore_signal(barrier, inc=1, device_id={"ep": (e + k) % EP, "fsdp": f}, device_id_type=MESH)

    def load(d):
        return pltpu.make_async_copy(train.at[d], x.at[d], load_sem.at[d])

    @pl.loop(0, N)
    def _(k):
        load(peer((HALF + k) % N)).start()

    loads = [pltpu.make_async_copy(ref, small.at[k], load_sem.at[N + k]) for k, ref in enumerate((weight, gain))]
    for copy in loads:
        copy.start()
    for copy in loads:
        copy.wait()
    mine = (small[0] * small[1]).astype(jnp.bfloat16).astype(jnp.float32)
    routed[pl.ds(e, 1), :] = mine

    def squares(d, coded_rows):
        load(d).wait()
        lanes = []
        for k in range(4):
            block = x[d, 128 * k : min(128 * k + 128, ROWS), :]
            column = jnp.sum(block * block, axis=1, keepdims=True)
            lanes.append(to_lanes(column))
            n = min(coded_rows - 128 * k, block.shape[0])
            if n > 0:
                rows16[d, 128 * k : 128 * k + n, :] = code(block[:n], column[:n])
        part[d // HALF, d % HALF] = jnp.concatenate(lanes, axis=0)

    squares(partner, ROWS)

    @pl.loop(HALF + 1, N)
    def _(k):
        squares(peer(k), EARLY[-1])

    pl.semaphore_wait(barrier, HALF + EP - 1)

    pl.semaphore_signal(far_sem, inc=1, device_id=to(partner), device_id_type=MESH)
    send(part.at[partner // HALF, partner % HALF], norms.at[place], send_sem.at[4], recv_sem.at[8], to(partner)).start()
    send(rows16.at[partner], coded.at[place], send_sem.at[3], recv_sem.at[7], to(partner)).start()

    @pl.loop(0, HALF)
    def _(k):
        squares(peer(k), 0)

    @pl.loop(1, HALF)
    def _(k):
        d = peer(k)
        send(part.at[:, d % HALF], parts.at[:, place], send_sem.at[0], recv_sem.at[0], to(d)).start()

    @pl.loop(1, EP)
    def _(k):
        send(
            routed.at[pl.ds(e, 1)], routed.at[pl.ds(e, 1)], send_sem.at[5], recv_sem.at[5], {"ep": (e + k) % EP, "fsdp": f}
        ).start()

    def early(begin, end):
        rows = pl.ds(begin, end - begin)

        @pl.loop(HALF + 1, N)
        def _(k):
            d = peer(k)
            send(rows16.at[d, rows], coded.at[place, rows], send_sem.at[3], recv_sem.at[4], to(d)).start()
            if begin == 0:
                row = pl.ds(0, 1)
                send(part.at[d // HALF, d % HALF, row], norms.at[place, row], send_sem.at[4], recv_sem.at[6], to(d)).start()

    pl.semaphore_wait(far_sem, 1)
    early(0, EARLY[0])

    parts[:, place] = part[:, place]
    drain(parts.at[:, pl.ds(0, HALF - 1)], recv_sem.at[0])
    plane = jnp.sum(parts[...], axis=1)
    sums[0:4, :] = plane[0]
    sums[4:8, :] = plane[1]
    drain(routed.at[pl.ds(0, EP - 1)], recv_sem.at[5])
    sums[8:16, :] = routed[...]
    send(sums, others, send_sem.at[1], recv_sem.at[1], to(partner)).start()

    early(EARLY[0], EARLY[1])
    drain(sums, recv_sem.at[1])
    root = jnp.sqrt(sums[0:8, :] + others[0:8, :])
    news[0:8, :] = 1.0 / root
    first = half == 0
    news[8:16, :] = jnp.where(first, sums[8:16, :], others[8:16, :])
    news[16:24, :] = jnp.where(first, others[8:16, :], sums[8:16, :])

    @pl.loop(1, HALF)
    def _(k):
        send(news, told.at[place], send_sem.at[2], recv_sem.at[2], to(peer(k))).start()

    told[place] = news[...]
    own = jnp.where(first, root[0:4], root[4:8])
    for k in range(4):
        n = min(128, ROWS - 128 * k)
        scale[:, 128 * k : 128 * k + n] = own[k : k + 1, :n]

    drain(told.at[pl.ds(0, HALF - 1)], recv_sem.at[2])

    columns = pl.ds(pl.multiple_of(f * COLS, COLS), COLS)

    def ready_rows(d, first, last):
        return stacked(
            [
                (
                    x[d, 128 * k + start : 128 * k + start + n, :]
                    * to_column(told[d % HALF, pl.ds(4 * (d // HALF) + k, 1), :], start, n)
                ).astype(jnp.bfloat16)
                for k, start, n in blocks_of(first, last)
            ]
        )

    def exact(begin, end, first, last, number):
        rows = pl.ds(first, last - first)

        @pl.loop(begin, end)
        def _(k):
            d = peer(k)
            rows16[d, first:last, :] = ready_rows(d, first, last)
            send(rows16.at[d, rows], ready.at[rows, columns], send_sem.at[3], recv_sem.at[number], to(d)).start()

    for i in range(len(CUTS) - 1):
        exact(HALF + 1, N, max(CUTS[i], EARLY[1]), CUTS[i + 1], 3)
        exact(1, HALF, CUTS[i], CUTS[i + 1], 9)
    ready[:, columns] = ready_rows(f, 0, ROWS)

    for h in range(2):
        for p in range(HALF):
            at = COLS * (HALF * h + p)
            router[:, at : at + COLS] = told[p, 8 + 8 * h : 16 + 8 * h, :].astype(jnp.bfloat16)

    inverse = 1.0 / own

    def decoded(d, last):
        p = d % HALF
        at = pl.ds(pl.multiple_of(d * COLS, COLS), COLS)
        for k, start, n in blocks_of(0, last):
            factor = jnp.sqrt(jnp.maximum(norms[p, k : k + 1, :], TINY)) * inverse[k : k + 1] * (1.0 / SPREAD)
            ready[128 * k : 128 * k + n, at] = decode(coded[p, 128 * k : 128 * k + n, :], to_column(factor, start, n))

    others_far = pl.ds(0, HALF - 1)
    drain(norms.at[0], recv_sem.at[8])
    drain(coded.at[0], recv_sem.at[7])
    decoded(partner, ROWS)
    drain(norms.at[others_far, pl.ds(0, 1)], recv_sem.at[6])
    drain(coded.at[others_far, pl.ds(0, EARLY[1])], recv_sem.at[4])

    @pl.loop(HALF + 1, N)
    def _(k):
        decoded(peer(k), EARLY[1])

    drain(rows16.at[others_far, pl.ds(0, ROWS - EARLY[1])], recv_sem.at[3])
    drain(rows16.at[others_far], recv_sem.at[9])
    drain(parts.at[:, pl.ds(0, HALF - 1)], send_sem.at[0])
    drain(sums, send_sem.at[1])
    drain(told.at[pl.ds(0, HALF - 1)], send_sem.at[2])
    drain(rows16.at[pl.ds(0, N - 1)], send_sem.at[3])
    drain(norms.at[0], send_sem.at[4])
    drain(norms.at[others_far, pl.ds(0, 1)], send_sem.at[4])
    drain(routed.at[pl.ds(0, EP - 1)], send_sem.at[5])


def store(ready, scale, router, ready_out, scale_out, router_out, sem):
    rows = ROWS // STORES
    copies = [pltpu.make_async_copy(scale, scale_out, sem.at[0]), pltpu.make_async_copy(router, router_out, sem.at[1])]
    for k in range(STORES):
        piece = pl.ds(rows * k, rows)
        copies.append(pltpu.make_async_copy(ready.at[piece], ready_out.at[piece], sem.at[2 + k]))
    for copy in copies:
        copy.start()
    for copy in copies:
        copy.wait()


def body(train_down, router_weight, router_gain):
    ready, scale, router = pl.pallas_call(
        exchange,
        out_shape=(
            jax.ShapeDtypeStruct((ROWS, N * COLS), jnp.bfloat16),
            jax.ShapeDtypeStruct((1, ROWS), jnp.float32),
            jax.ShapeDtypeStruct((EP, N * COLS), jnp.bfloat16),
        ),
        in_specs=[pl.BlockSpec(memory_space=pltpu.HBM)] * 3,
        out_specs=[pl.BlockSpec(memory_space=pltpu.VMEM)] * 3,
        scratch_shapes=[
            pltpu.VMEM((N, ROWS, COLS), jnp.float32),
            pltpu.VMEM((2, 1, COLS), jnp.float32),
            pltpu.VMEM((2, HALF, 4, 128), jnp.float32),
            pltpu.VMEM((2, HALF, 4, 128), jnp.float32),
            pltpu.VMEM((HALF, 4, 128), jnp.float32),
            pltpu.VMEM((EP, COLS), jnp.float32),
            pltpu.VMEM((16, 128), jnp.float32),
            pltpu.VMEM((16, 128), jnp.float32),
            pltpu.VMEM((24, 128), jnp.float32),
            pltpu.VMEM((HALF, 24, 128), jnp.float32),
            pltpu.VMEM((N, ROWS, COLS), jnp.bfloat16),
            pltpu.VMEM((HALF, ROWS, COLS), jnp.bfloat16),
            pltpu.SemaphoreType.DMA((N + 2,)),
            pltpu.SemaphoreType.DMA((6,)),
            pltpu.SemaphoreType.DMA((10,)),
            pltpu.SemaphoreType.REGULAR,
        ],
        compiler_params=pltpu.CompilerParams(
            collective_id=0, has_side_effects=True, vmem_limit_bytes=32 * 2**20
        ),
        name="exchange",
    )(
        *(
            pltpu.with_memory_space_constraint(array, pltpu.HBM)
            for array in (
                train_down.reshape(N, ROWS, COLS),
                router_weight.reshape(1, COLS),
                router_gain.reshape(1, COLS),
            )
        )
    )
    ready, scale, router = pl.pallas_call(
        store,
        out_shape=(
            jax.ShapeDtypeStruct(ready.shape, ready.dtype),
            jax.ShapeDtypeStruct(scale.shape, scale.dtype),
            jax.ShapeDtypeStruct(router.shape, router.dtype),
        ),
        in_specs=[pl.BlockSpec(memory_space=pltpu.VMEM)] * 3,
        out_specs=[pl.BlockSpec(memory_space=pltpu.HBM)] * 3,
        scratch_shapes=[pltpu.SemaphoreType.DMA((2 + STORES,))],
        compiler_params=pltpu.CompilerParams(vmem_limit_bytes=2**20),
        name="store",
    )(ready, scale, router)
    return ready[None], scale, router.T


def solution(mesh):
    in_specs = (P("ep", None, "fsdp"), P("fsdp", "ep"), P("fsdp"))
    out_specs = (P("ep", "fsdp", None), P("ep", "fsdp"), P())
    return jax.shard_map(body, mesh=mesh, in_specs=in_specs, out_specs=out_specs, check_vma=False)
```

```python
import jax
import jax.numpy as jnp
from jax import lax
from jax.experimental import pallas as pl
from jax.experimental.pallas import tpu as pltpu
from jax.sharding import PartitionSpec as P

MESH = pl.DeviceIdType.MESH
N = 32
EP = 8
ROWS = 448
COLS = 128
STORES = 7
HALF = N // 2
CUTS = (0, 256, 448)
EARLY = (48, 112)
POWER = 15
SPREAD = 2.0**8.4
TINY = 1e-37


def peer(k):
    f = lax.axis_index("fsdp")
    h = (f // 16 + k // 16) % 2
    y = ((f // 4) % 4 + (k // 4) % 4) % 4
    x = (f % 4 + k % 4) % 4
    return h * 16 + y * 4 + x


def send(src, dst, send_sem, recv_sem, device):
    return pltpu.make_async_remote_copy(
        src_ref=src,
        dst_ref=dst,
        send_sem=send_sem,
        recv_sem=recv_sem,
        device_id=device,
        device_id_type=MESH,
    )


def drain(ref, sem):
    pltpu.make_async_copy(ref, ref, sem).wait()


def eye():
    return lax.broadcasted_iota(jnp.int32, (128, 128), 0) == lax.broadcasted_iota(jnp.int32, (128, 128), 1)


def to_lanes(column):
    n = column.shape[0]
    return jnp.sum(jnp.where(eye()[:n], column, 0.0), axis=0, keepdims=True)


def to_column(row, start, n):
    return jnp.sum(jnp.where(eye()[start : start + n], row, 0.0), axis=1, keepdims=True)


def code(block, squares):
    u = block * (lax.rsqrt(jnp.maximum(squares, TINY)) * SPREAD)
    u2 = u * u
    u4 = u2 * u2
    return (u4 * u4 * u4 * u2 * u).astype(jnp.bfloat16)


def decode(coded, factor):
    y = coded.astype(jnp.float32)
    size = jnp.exp(jnp.log(jnp.maximum(jnp.abs(y), TINY)) * (1.0 / POWER)) * factor
    return jnp.where(y > 0.0, size, jnp.where(y < 0.0, -size, 0.0 * factor)).astype(jnp.bfloat16)


def blocks_of(first, last):
    row = first
    while row < last:
        k, start = row // 128, row % 128
        n = min(128 - start, last - row)
        yield k, start, n
        row += n


def stacked(blocks):
    return jnp.concatenate(blocks, axis=0) if len(blocks) > 1 else blocks[0]


def exchange(
    train, weight, gain, ready, scale, router,
    x, small, part, parts, norms, routed, sums, others, news, told, rows16, coded,
    load_sem, send_sem, recv_sem, far_sem,
):
    e, f = lax.axis_index("ep"), lax.axis_index("fsdp")
    half, place = f // HALF, f % HALF
    partner = peer(HALF)

    def to(device):
        return {"ep": e, "fsdp": device}

    def load(d):
        return pltpu.make_async_copy(train.at[d], x.at[d], load_sem.at[d])

    load(partner).start()
    loads = [pltpu.make_async_copy(ref, small.at[k], load_sem.at[N + k]) for k, ref in enumerate((weight, gain))]
    for copy in loads:
        copy.start()

    barrier = pltpu.get_barrier_semaphore()

    @pl.loop(1, HALF + 1)
    def _(k):
        pl.semaphore_signal(barrier, inc=1, device_id=to(peer(k)), device_id_type=MESH)

    @pl.loop(1, EP)
    def _(k):
        pl.semaphore_signal(barrier, inc=1, device_id={"ep": (e + k) % EP, "fsdp": f}, device_id_type=MESH)

    @pl.loop(1, N)
    def _(k):
        load(peer((HALF + k) % N)).start()

    def squares(d, coded_rows):
        load(d).wait()
        lanes = []
        for k in range(4):
            block = x[d, 128 * k : min(128 * k + 128, ROWS), :]
            column = jnp.sum(block * block, axis=1, keepdims=True)
            lanes.append(to_lanes(column))
            n = min(coded_rows - 128 * k, block.shape[0])
            if n > 0:
                rows16[d, 128 * k : 128 * k + n, :] = code(block[:n], column[:n])
        part[d // HALF, d % HALF] = jnp.concatenate(lanes, axis=0)

    squares(partner, ROWS)

    pl.semaphore_wait(barrier, HALF + EP - 1)

    pl.semaphore_signal(far_sem, inc=1, device_id=to(partner), device_id_type=MESH)
    send(part.at[partner // HALF, partner % HALF], norms.at[place], send_sem.at[4], recv_sem.at[8], to(partner)).start()
    send(rows16.at[partner], coded.at[place], send_sem.at[3], recv_sem.at[7], to(partner)).start()

    @pl.loop(HALF + 1, N)
    def _(k):
        squares(peer(k), EARLY[-1])

    @pl.loop(0, HALF)
    def _(k):
        squares(peer(k), 0)

    for copy in loads:
        copy.wait()
    mine = (small[0] * small[1]).astype(jnp.bfloat16).astype(jnp.float32)
    routed[pl.ds(e, 1), :] = mine

    @pl.loop(1, HALF)
    def _(k):
        d = peer(k)
        send(part.at[:, d % HALF], parts.at[:, place], send_sem.at[0], recv_sem.at[0], to(d)).start()

    @pl.loop(1, EP)
    def _(k):
        send(
            routed.at[pl.ds(e, 1)], routed.at[pl.ds(e, 1)], send_sem.at[5], recv_sem.at[5], {"ep": (e + k) % EP, "fsdp": f}
        ).start()

    def early(begin, end):
        rows = pl.ds(begin, end - begin)

        @pl.loop(HALF + 1, N)
        def _(k):
            d = peer(k)
            send(rows16.at[d, rows], coded.at[place, rows], send_sem.at[3], recv_sem.at[4], to(d)).start()
            if begin == 0:
                row = pl.ds(0, 1)
                send(part.at[d // HALF, d % HALF, row], norms.at[place, row], send_sem.at[4], recv_sem.at[6], to(d)).start()

    pl.semaphore_wait(far_sem, 1)
    early(0, EARLY[0])

    parts[:, place] = part[:, place]
    drain(parts.at[:, pl.ds(0, HALF - 1)], recv_sem.at[0])
    plane = jnp.sum(parts[...], axis=1)
    sums[0:4, :] = plane[0]
    sums[4:8, :] = plane[1]
    drain(routed.at[pl.ds(0, EP - 1)], recv_sem.at[5])
    sums[8:16, :] = routed[...]
    send(sums, others, send_sem.at[1], recv_sem.at[1], to(partner)).start()

    early(EARLY[0], EARLY[1])
    drain(sums, recv_sem.at[1])
    root = jnp.sqrt(sums[0:8, :] + others[0:8, :])
    news[0:8, :] = 1.0 / root
    first = half == 0
    news[8:16, :] = jnp.where(first, sums[8:16, :], others[8:16, :])
    news[16:24, :] = jnp.where(first, others[8:16, :], sums[8:16, :])

    @pl.loop(1, HALF)
    def _(k):
        send(news, told.at[place], send_sem.at[2], recv_sem.at[2], to(peer(k))).start()

    told[place] = news[...]
    own = jnp.where(first, root[0:4], root[4:8])
    for k in range(4):
        n = min(128, ROWS - 128 * k)
        scale[:, 128 * k : 128 * k + n] = own[k : k + 1, :n]

    drain(told.at[pl.ds(0, HALF - 1)], recv_sem.at[2])

    columns = pl.ds(pl.multiple_of(f * COLS, COLS), COLS)

    def ready_rows(d, first, last):
        return stacked(
            [
                (
                    x[d, 128 * k + start : 128 * k + start + n, :]
                    * to_column(told[d % HALF, pl.ds(4 * (d // HALF) + k, 1), :], start, n)
                ).astype(jnp.bfloat16)
                for k, start, n in blocks_of(first, last)
            ]
        )

    def exact(begin, end, first, last, number):
        rows = pl.ds(first, last - first)

        @pl.loop(begin, end)
        def _(k):
            d = peer(k)
            rows16[d, first:last, :] = ready_rows(d, first, last)
            send(rows16.at[d, rows], ready.at[rows, columns], send_sem.at[3], recv_sem.at[number], to(d)).start()

    for i in range(len(CUTS) - 1):
        exact(HALF + 1, N, max(CUTS[i], EARLY[1]), CUTS[i + 1], 3)
        exact(1, HALF, CUTS[i], CUTS[i + 1], 9)
    ready[:, columns] = ready_rows(f, 0, ROWS)

    for h in range(2):
        for p in range(HALF):
            at = COLS * (HALF * h + p)
            router[:, at : at + COLS] = told[p, 8 + 8 * h : 16 + 8 * h, :].astype(jnp.bfloat16)

    inverse = 1.0 / own

    def decoded(d, last):
        p = d % HALF
        at = pl.ds(pl.multiple_of(d * COLS, COLS), COLS)
        for k, start, n in blocks_of(0, last):
            factor = jnp.sqrt(jnp.maximum(norms[p, k : k + 1, :], TINY)) * inverse[k : k + 1] * (1.0 / SPREAD)
            ready[128 * k : 128 * k + n, at] = decode(coded[p, 128 * k : 128 * k + n, :], to_column(factor, start, n))

    others_far = pl.ds(0, HALF - 1)
    drain(norms.at[0], recv_sem.at[8])
    drain(coded.at[0], recv_sem.at[7])
    decoded(partner, ROWS)
    drain(norms.at[others_far, pl.ds(0, 1)], recv_sem.at[6])
    drain(coded.at[others_far, pl.ds(0, EARLY[1])], recv_sem.at[4])

    @pl.loop(HALF + 1, N)
    def _(k):
        decoded(peer(k), EARLY[1])

    drain(rows16.at[others_far, pl.ds(0, ROWS - EARLY[1])], recv_sem.at[3])
    drain(rows16.at[others_far], recv_sem.at[9])
    drain(parts.at[:, pl.ds(0, HALF - 1)], send_sem.at[0])
    drain(sums, send_sem.at[1])
    drain(told.at[pl.ds(0, HALF - 1)], send_sem.at[2])
    drain(rows16.at[pl.ds(0, N - 1)], send_sem.at[3])
    drain(norms.at[0], send_sem.at[4])
    drain(norms.at[others_far, pl.ds(0, 1)], send_sem.at[4])
    drain(routed.at[pl.ds(0, EP - 1)], send_sem.at[5])


def store(ready, scale, router, ready_out, scale_out, router_out, sem):
    rows = ROWS // STORES
    copies = [pltpu.make_async_copy(scale, scale_out, sem.at[0]), pltpu.make_async_copy(router, router_out, sem.at[1])]
    for k in range(STORES):
        piece = pl.ds(rows * k, rows)
        copies.append(pltpu.make_async_copy(ready.at[piece], ready_out.at[piece], sem.at[2 + k]))
    for copy in copies:
        copy.start()
    for copy in copies:
        copy.wait()


def body(train_down, router_weight, router_gain):
    ready, scale, router = pl.pallas_call(
        exchange,
        out_shape=(
            jax.ShapeDtypeStruct((ROWS, N * COLS), jnp.bfloat16),
            jax.ShapeDtypeStruct((1, ROWS), jnp.float32),
            jax.ShapeDtypeStruct((EP, N * COLS), jnp.bfloat16),
        ),
        in_specs=[pl.BlockSpec(memory_space=pltpu.HBM)] * 3,
        out_specs=[pl.BlockSpec(memory_space=pltpu.VMEM)] * 3,
        scratch_shapes=[
            pltpu.VMEM((N, ROWS, COLS), jnp.float32),
            pltpu.VMEM((2, 1, COLS), jnp.float32),
            pltpu.VMEM((2, HALF, 4, 128), jnp.float32),
            pltpu.VMEM((2, HALF, 4, 128), jnp.float32),
            pltpu.VMEM((HALF, 4, 128), jnp.float32),
            pltpu.VMEM((EP, COLS), jnp.float32),
            pltpu.VMEM((16, 128), jnp.float32),
            pltpu.VMEM((16, 128), jnp.float32),
            pltpu.VMEM((24, 128), jnp.float32),
            pltpu.VMEM((HALF, 24, 128), jnp.float32),
            pltpu.VMEM((N, ROWS, COLS), jnp.bfloat16),
            pltpu.VMEM((HALF, ROWS, COLS), jnp.bfloat16),
            pltpu.SemaphoreType.DMA((N + 2,)),
            pltpu.SemaphoreType.DMA((6,)),
            pltpu.SemaphoreType.DMA((10,)),
            pltpu.SemaphoreType.REGULAR,
        ],
        compiler_params=pltpu.CompilerParams(
            collective_id=0, has_side_effects=True, vmem_limit_bytes=32 * 2**20
        ),
        name="exchange",
    )(
        *(
            pltpu.with_memory_space_constraint(array, pltpu.HBM)
            for array in (
                train_down.reshape(N, ROWS, COLS),
                router_weight.reshape(1, COLS),
                router_gain.reshape(1, COLS),
            )
        )
    )
    ready, scale, router = pl.pallas_call(
        store,
        out_shape=(
            jax.ShapeDtypeStruct(ready.shape, ready.dtype),
            jax.ShapeDtypeStruct(scale.shape, scale.dtype),
            jax.ShapeDtypeStruct(router.shape, router.dtype),
        ),
        in_specs=[pl.BlockSpec(memory_space=pltpu.VMEM)] * 3,
        out_specs=[pl.BlockSpec(memory_space=pltpu.HBM)] * 3,
        scratch_shapes=[pltpu.SemaphoreType.DMA((2 + STORES,))],
        compiler_params=pltpu.CompilerParams(vmem_limit_bytes=2**20),
        name="store",
    )(ready, scale, router)
    return ready[None], scale, router.T


def solution(mesh):
    in_specs = (P("ep", None, "fsdp"), P("fsdp", "ep"), P("fsdp"))
    out_specs = (P("ep", "fsdp", None), P("ep", "fsdp"), P())
    return jax.shard_map(body, mesh=mesh, in_specs=in_specs, out_specs=out_specs, check_vma=False)
```

```python
import jax
import jax.numpy as jnp
from jax import lax
from jax.experimental import pallas as pl
from jax.experimental.pallas import tpu as pltpu
from jax.sharding import PartitionSpec as P

MESH = pl.DeviceIdType.MESH
N = 32
EP = 8
ROWS = 448
COLS = 128
STORES = 7
HALF = N // 2
CUTS = (0, 256, 448)
EARLY = (64, 112)
POWER = 15
SPREAD = 2.0**8.4
TINY = 1e-37


def peer(k):
    f = lax.axis_index("fsdp")
    h = (f // 16 + k // 16) % 2
    y = ((f // 4) % 4 + (k // 4) % 4) % 4
    x = (f % 4 + k % 4) % 4
    return h * 16 + y * 4 + x


def send(src, dst, send_sem, recv_sem, device):
    return pltpu.make_async_remote_copy(
        src_ref=src,
        dst_ref=dst,
        send_sem=send_sem,
        recv_sem=recv_sem,
        device_id=device,
        device_id_type=MESH,
    )


def drain(ref, sem):
    pltpu.make_async_copy(ref, ref, sem).wait()


def eye():
    return lax.broadcasted_iota(jnp.int32, (128, 128), 0) == lax.broadcasted_iota(jnp.int32, (128, 128), 1)


def to_lanes(column):
    n = column.shape[0]
    return jnp.sum(jnp.where(eye()[:n], column, 0.0), axis=0, keepdims=True)


def to_column(row, start, n):
    return jnp.sum(jnp.where(eye()[start : start + n], row, 0.0), axis=1, keepdims=True)


def code(block, squares):
    u = block * (lax.rsqrt(jnp.maximum(squares, TINY)) * SPREAD)
    u2 = u * u
    u4 = u2 * u2
    return (u4 * u4 * u4 * u2 * u).astype(jnp.bfloat16)


def decode(coded, factor):
    y = coded.astype(jnp.float32)
    size = jnp.exp(jnp.log(jnp.maximum(jnp.abs(y), TINY)) * (1.0 / POWER)) * factor
    return jnp.where(y > 0.0, size, jnp.where(y < 0.0, -size, 0.0 * factor)).astype(jnp.bfloat16)


def blocks_of(first, last):
    row = first
    while row < last:
        k, start = row // 128, row % 128
        n = min(128 - start, last - row)
        yield k, start, n
        row += n


def stacked(blocks):
    return jnp.concatenate(blocks, axis=0) if len(blocks) > 1 else blocks[0]


def exchange(
    train, weight, gain, ready, scale, router,
    x, small, part, parts, norms, routed, sums, others, news, told, rows16, coded,
    load_sem, send_sem, recv_sem, far_sem,
):
    e, f = lax.axis_index("ep"), lax.axis_index("fsdp")
    half, place = f // HALF, f % HALF
    partner = peer(HALF)

    def to(device):
        return {"ep": e, "fsdp": device}

    def load(d):
        return pltpu.make_async_copy(train.at[d], x.at[d], load_sem.at[d])

    load(partner).start()
    loads = [pltpu.make_async_copy(ref, small.at[k], load_sem.at[N + k]) for k, ref in enumerate((weight, gain))]
    for copy in loads:
        copy.start()

    barrier = pltpu.get_barrier_semaphore()

    pl.semaphore_signal(barrier, inc=1, device_id=to(partner), device_id_type=MESH)

    @pl.loop(1, HALF)
    def _(k):
        pl.semaphore_signal(barrier, inc=1, device_id=to(peer(k)), device_id_type=MESH)

    @pl.loop(1, EP)
    def _(k):
        pl.semaphore_signal(barrier, inc=1, device_id={"ep": (e + k) % EP, "fsdp": f}, device_id_type=MESH)

    @pl.loop(1, N)
    def _(k):
        load(peer((HALF + k) % N)).start()

    def squares(d, coded_rows):
        load(d).wait()
        lanes = []
        for k in range(4):
            block = x[d, 128 * k : min(128 * k + 128, ROWS), :]
            column = jnp.sum(block * block, axis=1, keepdims=True)
            lanes.append(to_lanes(column))
            n = min(coded_rows - 128 * k, block.shape[0])
            if n > 0:
                rows16[d, 128 * k : 128 * k + n, :] = code(block[:n], column[:n])
        part[d // HALF, d % HALF] = jnp.concatenate(lanes, axis=0)

    squares(partner, ROWS)

    pl.semaphore_wait(barrier, HALF + EP - 1)

    pl.semaphore_signal(far_sem, inc=1, device_id=to(partner), device_id_type=MESH)
    send(part.at[partner // HALF, partner % HALF], norms.at[place], send_sem.at[4], recv_sem.at[8], to(partner)).start()
    send(rows16.at[partner], coded.at[place], send_sem.at[3], recv_sem.at[7], to(partner)).start()

    @pl.loop(HALF + 1, N)
    def _(k):
        squares(peer(k), EARLY[-1])

    @pl.loop(0, HALF)
    def _(k):
        squares(peer(k), 0)

    for copy in loads:
        copy.wait()
    mine = (small[0] * small[1]).astype(jnp.bfloat16).astype(jnp.float32)
    routed[pl.ds(e, 1), :] = mine

    @pl.loop(1, HALF)
    def _(k):
        d = peer(k)
        send(part.at[:, d % HALF], parts.at[:, place], send_sem.at[0], recv_sem.at[0], to(d)).start()

    @pl.loop(1, EP)
    def _(k):
        send(
            routed.at[pl.ds(e, 1)], routed.at[pl.ds(e, 1)], send_sem.at[5], recv_sem.at[5], {"ep": (e + k) % EP, "fsdp": f}
        ).start()

    def early(begin, end):
        rows = pl.ds(begin, end - begin)

        @pl.loop(HALF + 1, N)
        def _(k):
            d = peer(k)
            send(rows16.at[d, rows], coded.at[place, rows], send_sem.at[3], recv_sem.at[4], to(d)).start()
            if begin == 0:
                row = pl.ds(0, 1)
                send(part.at[d // HALF, d % HALF, row], norms.at[place, row], send_sem.at[4], recv_sem.at[6], to(d)).start()

    pl.semaphore_wait(far_sem, 1)
    early(0, EARLY[0])

    parts[:, place] = part[:, place]
    drain(parts.at[:, pl.ds(0, HALF - 1)], recv_sem.at[0])
    plane = jnp.sum(parts[...], axis=1)
    sums[0:4, :] = plane[0]
    sums[4:8, :] = plane[1]
    drain(routed.at[pl.ds(0, EP - 1)], recv_sem.at[5])
    sums[8:16, :] = routed[...]
    send(sums, others, send_sem.at[1], recv_sem.at[1], to(partner)).start()

    early(EARLY[0], EARLY[1])
    drain(sums, recv_sem.at[1])
    root = jnp.sqrt(sums[0:8, :] + others[0:8, :])
    news[0:8, :] = 1.0 / root
    first = half == 0
    news[8:16, :] = jnp.where(first, sums[8:16, :], others[8:16, :])
    news[16:24, :] = jnp.where(first, others[8:16, :], sums[8:16, :])

    @pl.loop(1, HALF)
    def _(k):
        send(news, told.at[place], send_sem.at[2], recv_sem.at[2], to(peer(k))).start()

    told[place] = news[...]
    own = jnp.where(first, root[0:4], root[4:8])
    for k in range(4):
        n = min(128, ROWS - 128 * k)
        scale[:, 128 * k : 128 * k + n] = own[k : k + 1, :n]

    drain(told.at[pl.ds(0, HALF - 1)], recv_sem.at[2])

    columns = pl.ds(pl.multiple_of(f * COLS, COLS), COLS)

    def ready_rows(d, first, last):
        return stacked(
            [
                (
                    x[d, 128 * k + start : 128 * k + start + n, :]
                    * to_column(told[d % HALF, pl.ds(4 * (d // HALF) + k, 1), :], start, n)
                ).astype(jnp.bfloat16)
                for k, start, n in blocks_of(first, last)
            ]
        )

    def exact(begin, end, first, last, number):
        rows = pl.ds(first, last - first)

        @pl.loop(begin, end)
        def _(k):
            d = peer(k)
            rows16[d, first:last, :] = ready_rows(d, first, last)
            send(rows16.at[d, rows], ready.at[rows, columns], send_sem.at[3], recv_sem.at[number], to(d)).start()

    for i in range(len(CUTS) - 1):
        exact(HALF + 1, N, max(CUTS[i], EARLY[1]), CUTS[i + 1], 3)
        exact(1, HALF, CUTS[i], CUTS[i + 1], 9)
    ready[:, columns] = ready_rows(f, 0, ROWS)

    for h in range(2):
        for p in range(HALF):
            at = COLS * (HALF * h + p)
            router[:, at : at + COLS] = told[p, 8 + 8 * h : 16 + 8 * h, :].astype(jnp.bfloat16)

    inverse = 1.0 / own

    def decoded(d, last):
        p = d % HALF
        at = pl.ds(pl.multiple_of(d * COLS, COLS), COLS)
        for k, start, n in blocks_of(0, last):
            factor = jnp.sqrt(jnp.maximum(norms[p, k : k + 1, :], TINY)) * inverse[k : k + 1] * (1.0 / SPREAD)
            ready[128 * k : 128 * k + n, at] = decode(coded[p, 128 * k : 128 * k + n, :], to_column(factor, start, n))

    others_far = pl.ds(0, HALF - 1)
    drain(norms.at[0], recv_sem.at[8])
    drain(coded.at[0], recv_sem.at[7])
    decoded(partner, ROWS)
    drain(norms.at[others_far, pl.ds(0, 1)], recv_sem.at[6])
    drain(coded.at[others_far, pl.ds(0, EARLY[1])], recv_sem.at[4])

    @pl.loop(HALF + 1, N)
    def _(k):
        decoded(peer(k), EARLY[1])

    drain(rows16.at[others_far, pl.ds(0, ROWS - EARLY[1])], recv_sem.at[3])
    drain(rows16.at[others_far], recv_sem.at[9])
    drain(parts.at[:, pl.ds(0, HALF - 1)], send_sem.at[0])
    drain(sums, send_sem.at[1])
    drain(told.at[pl.ds(0, HALF - 1)], send_sem.at[2])
    drain(rows16.at[pl.ds(0, N - 1)], send_sem.at[3])
    drain(norms.at[0], send_sem.at[4])
    drain(norms.at[others_far, pl.ds(0, 1)], send_sem.at[4])
    drain(routed.at[pl.ds(0, EP - 1)], send_sem.at[5])


def store(ready, scale, router, ready_out, scale_out, router_out, sem):
    rows = ROWS // STORES
    copies = [pltpu.make_async_copy(scale, scale_out, sem.at[0]), pltpu.make_async_copy(router, router_out, sem.at[1])]
    for k in range(STORES):
        piece = pl.ds(rows * k, rows)
        copies.append(pltpu.make_async_copy(ready.at[piece], ready_out.at[piece], sem.at[2 + k]))
    for copy in copies:
        copy.start()
    for copy in copies:
        copy.wait()


def body(train_down, router_weight, router_gain):
    ready, scale, router = pl.pallas_call(
        exchange,
        out_shape=(
            jax.ShapeDtypeStruct((ROWS, N * COLS), jnp.bfloat16),
            jax.ShapeDtypeStruct((1, ROWS), jnp.float32),
            jax.ShapeDtypeStruct((EP, N * COLS), jnp.bfloat16),
        ),
        in_specs=[pl.BlockSpec(memory_space=pltpu.HBM)] * 3,
        out_specs=[pl.BlockSpec(memory_space=pltpu.VMEM)] * 3,
        scratch_shapes=[
            pltpu.VMEM((N, ROWS, COLS), jnp.float32),
            pltpu.VMEM((2, 1, COLS), jnp.float32),
            pltpu.VMEM((2, HALF, 4, 128), jnp.float32),
            pltpu.VMEM((2, HALF, 4, 128), jnp.float32),
            pltpu.VMEM((HALF, 4, 128), jnp.float32),
            pltpu.VMEM((EP, COLS), jnp.float32),
            pltpu.VMEM((16, 128), jnp.float32),
            pltpu.VMEM((16, 128), jnp.float32),
            pltpu.VMEM((24, 128), jnp.float32),
            pltpu.VMEM((HALF, 24, 128), jnp.float32),
            pltpu.VMEM((N, ROWS, COLS), jnp.bfloat16),
            pltpu.VMEM((HALF, ROWS, COLS), jnp.bfloat16),
            pltpu.SemaphoreType.DMA((N + 2,)),
            pltpu.SemaphoreType.DMA((6,)),
            pltpu.SemaphoreType.DMA((10,)),
            pltpu.SemaphoreType.REGULAR,
        ],
        compiler_params=pltpu.CompilerParams(
            collective_id=0, has_side_effects=True, vmem_limit_bytes=32 * 2**20
        ),
        name="exchange",
    )(
        *(
            pltpu.with_memory_space_constraint(array, pltpu.HBM)
            for array in (
                train_down.reshape(N, ROWS, COLS),
                router_weight.reshape(1, COLS),
                router_gain.reshape(1, COLS),
            )
        )
    )
    ready, scale, router = pl.pallas_call(
        store,
        out_shape=(
            jax.ShapeDtypeStruct(ready.shape, ready.dtype),
            jax.ShapeDtypeStruct(scale.shape, scale.dtype),
            jax.ShapeDtypeStruct(router.shape, router.dtype),
        ),
        in_specs=[pl.BlockSpec(memory_space=pltpu.VMEM)] * 3,
        out_specs=[pl.BlockSpec(memory_space=pltpu.HBM)] * 3,
        scratch_shapes=[pltpu.SemaphoreType.DMA((2 + STORES,))],
        compiler_params=pltpu.CompilerParams(vmem_limit_bytes=2**20),
        name="store",
    )(ready, scale, router)
    return ready[None], scale, router.T


def solution(mesh):
    in_specs = (P("ep", None, "fsdp"), P("fsdp", "ep"), P("fsdp"))
    out_specs = (P("ep", "fsdp", None), P("ep", "fsdp"), P())
    return jax.shard_map(body, mesh=mesh, in_specs=in_specs, out_specs=out_specs, check_vma=False)
```

```python
import jax
import jax.numpy as jnp
from jax import lax
from jax.experimental import pallas as pl
from jax.experimental.pallas import tpu as pltpu
from jax.sharding import PartitionSpec as P

MESH = pl.DeviceIdType.MESH
N = 32
EP = 8
ROWS = 448
COLS = 128
STORES = 7
HALF = N // 2
CUTS = (0, 256, 448)
EARLY = (64, 112)
POWER = 15
SPREAD = 2.0**8.4
TINY = 1e-37


def peer(k):
    f = lax.axis_index("fsdp")
    h = (f // 16 + k // 16) % 2
    y = ((f // 4) % 4 + (k // 4) % 4) % 4
    x = (f % 4 + k % 4) % 4
    return h * 16 + y * 4 + x


def send(src, dst, send_sem, recv_sem, device):
    return pltpu.make_async_remote_copy(
        src_ref=src,
        dst_ref=dst,
        send_sem=send_sem,
        recv_sem=recv_sem,
        device_id=device,
        device_id_type=MESH,
    )


def drain(ref, sem):
    pltpu.make_async_copy(ref, ref, sem).wait()


def eye():
    return lax.broadcasted_iota(jnp.int32, (128, 128), 0) == lax.broadcasted_iota(jnp.int32, (128, 128), 1)


def to_lanes(column):
    n = column.shape[0]
    return jnp.sum(jnp.where(eye()[:n], column, 0.0), axis=0, keepdims=True)


def to_column(row, start, n):
    return jnp.sum(jnp.where(eye()[start : start + n], row, 0.0), axis=1, keepdims=True)


def code(block, squares):
    u = block * (lax.rsqrt(jnp.maximum(squares, TINY)) * SPREAD)
    u2 = u * u
    u4 = u2 * u2
    return (u4 * u4 * u4 * u2 * u).astype(jnp.bfloat16)


def decode(coded, factor):
    y = coded.astype(jnp.float32)
    size = jnp.exp(jnp.log(jnp.maximum(jnp.abs(y), TINY)) * (1.0 / POWER)) * factor
    return jnp.where(y > 0.0, size, jnp.where(y < 0.0, -size, 0.0 * factor)).astype(jnp.bfloat16)


def blocks_of(first, last):
    row = first
    while row < last:
        k, start = row // 128, row % 128
        n = min(128 - start, last - row)
        yield k, start, n
        row += n


def stacked(blocks):
    return jnp.concatenate(blocks, axis=0) if len(blocks) > 1 else blocks[0]


def exchange(
    train, weight, gain, ready, scale, router,
    x, small, part, parts, norms, routed, sums, others, news, told, rows16, coded,
    load_sem, send_sem, recv_sem, far_sem,
):
    e, f = lax.axis_index("ep"), lax.axis_index("fsdp")
    half, place = f // HALF, f % HALF
    partner = peer(HALF)

    def to(device):
        return {"ep": e, "fsdp": device}

    def load(d):
        return pltpu.make_async_copy(train.at[d], x.at[d], load_sem.at[d])

    load(partner).start()
    loads = [pltpu.make_async_copy(ref, small.at[k], load_sem.at[N + k]) for k, ref in enumerate((weight, gain))]
    for copy in loads:
        copy.start()

    barrier = pltpu.get_barrier_semaphore()

    pl.semaphore_signal(barrier, inc=1, device_id=to(partner), device_id_type=MESH)

    @pl.loop(1, HALF)
    def _(k):
        pl.semaphore_signal(barrier, inc=1, device_id=to(peer(k)), device_id_type=MESH)

    @pl.loop(1, EP)
    def _(k):
        pl.semaphore_signal(barrier, inc=1, device_id={"ep": (e + k) % EP, "fsdp": f}, device_id_type=MESH)

    @pl.loop(1, N)
    def _(k):
        load(peer((HALF + k) % N)).start()

    def squares(d, coded_rows):
        load(d).wait()
        lanes = []
        for k in range(4):
            block = x[d, 128 * k : min(128 * k + 128, ROWS), :]
            column = jnp.sum(block * block, axis=1, keepdims=True)
            lanes.append(to_lanes(column))
            n = min(coded_rows - 128 * k, block.shape[0])
            if n > 0:
                rows16[d, 128 * k : 128 * k + n, :] = code(block[:n], column[:n])
        part[d // HALF, d % HALF] = jnp.concatenate(lanes, axis=0)

    squares(partner, ROWS)

    pl.semaphore_wait(barrier, HALF + EP - 1)

    pl.semaphore_signal(far_sem, inc=1, device_id=to(partner), device_id_type=MESH)
    send(part.at[partner // HALF, partner % HALF], norms.at[place], send_sem.at[4], recv_sem.at[8], to(partner)).start()
    send(rows16.at[partner], coded.at[place], send_sem.at[3], recv_sem.at[7], to(partner)).start()

    @pl.loop(HALF + 1, N)
    def _(k):
        squares(peer(k), EARLY[-1])

    @pl.loop(0, HALF)
    def _(k):
        squares(peer(k), 0)

    for copy in loads:
        copy.wait()
    mine = (small[0] * small[1]).astype(jnp.bfloat16).astype(jnp.float32)
    routed[pl.ds(e, 1), :] = mine

    @pl.loop(1, HALF)
    def _(k):
        d = peer(k)
        send(part.at[:, d % HALF], parts.at[:, place], send_sem.at[0], recv_sem.at[0], to(d)).start()

    @pl.loop(1, EP)
    def _(k):
        send(
            routed.at[pl.ds(e, 1)], routed.at[pl.ds(e, 1)], send_sem.at[5], recv_sem.at[5], {"ep": (e + k) % EP, "fsdp": f}
        ).start()

    def early(begin, end):
        rows = pl.ds(begin, end - begin)

        @pl.loop(HALF + 1, N)
        def _(k):
            d = peer(k)
            send(rows16.at[d, rows], coded.at[place, rows], send_sem.at[3], recv_sem.at[4], to(d)).start()
            if begin == 0:
                row = pl.ds(0, 1)
                send(part.at[d // HALF, d % HALF, row], norms.at[place, row], send_sem.at[4], recv_sem.at[6], to(d)).start()

    pl.semaphore_wait(far_sem, 1)
    early(0, EARLY[0])

    parts[:, place] = part[:, place]
    drain(parts.at[:, pl.ds(0, HALF - 1)], recv_sem.at[0])
    plane = jnp.sum(parts[...], axis=1)
    sums[0:4, :] = plane[0]
    sums[4:8, :] = plane[1]
    drain(routed.at[pl.ds(0, EP - 1)], recv_sem.at[5])
    sums[8:16, :] = routed[...]
    send(sums, others, send_sem.at[1], recv_sem.at[1], to(partner)).start()

    early(EARLY[0], EARLY[1])
    drain(sums, recv_sem.at[1])
    root = jnp.sqrt(sums[0:8, :] + others[0:8, :])
    news[0:8, :] = 1.0 / root
    first = half == 0
    news[8:16, :] = jnp.where(first, sums[8:16, :], others[8:16, :])
    news[16:24, :] = jnp.where(first, others[8:16, :], sums[8:16, :])

    @pl.loop(1, HALF)
    def _(k):
        send(news, told.at[place], send_sem.at[2], recv_sem.at[2], to(peer(k))).start()

    told[place] = news[...]
    own = jnp.where(first, root[0:4], root[4:8])
    for k in range(4):
        n = min(128, ROWS - 128 * k)
        scale[:, 128 * k : 128 * k + n] = own[k : k + 1, :n]

    drain(told.at[pl.ds(0, HALF - 1)], recv_sem.at[2])

    columns = pl.ds(pl.multiple_of(f * COLS, COLS), COLS)

    def ready_rows(d, first, last):
        return stacked(
            [
                (
                    x[d, 128 * k + start : 128 * k + start + n, :]
                    * to_column(told[d % HALF, pl.ds(4 * (d // HALF) + k, 1), :], start, n)
                ).astype(jnp.bfloat16)
                for k, start, n in blocks_of(first, last)
            ]
        )

    def exact(begin, end, first, last, number):
        rows = pl.ds(first, last - first)

        @pl.loop(begin, end)
        def _(k):
            d = peer(k)
            rows16[d, first:last, :] = ready_rows(d, first, last)
            send(rows16.at[d, rows], ready.at[rows, columns], send_sem.at[3], recv_sem.at[number], to(d)).start()

    for i in range(len(CUTS) - 1):
        exact(HALF + 1, N, max(CUTS[i], EARLY[1]), CUTS[i + 1], 3)
    for i in range(len(CUTS) - 1):
        exact(1, HALF, CUTS[i], CUTS[i + 1], 9)
    ready[:, columns] = ready_rows(f, 0, ROWS)

    for h in range(2):
        for p in range(HALF):
            at = COLS * (HALF * h + p)
            router[:, at : at + COLS] = told[p, 8 + 8 * h : 16 + 8 * h, :].astype(jnp.bfloat16)

    inverse = 1.0 / own

    def decoded(d, last):
        p = d % HALF
        at = pl.ds(pl.multiple_of(d * COLS, COLS), COLS)
        for k, start, n in blocks_of(0, last):
            factor = jnp.sqrt(jnp.maximum(norms[p, k : k + 1, :], TINY)) * inverse[k : k + 1] * (1.0 / SPREAD)
            ready[128 * k : 128 * k + n, at] = decode(coded[p, 128 * k : 128 * k + n, :], to_column(factor, start, n))

    others_far = pl.ds(0, HALF - 1)
    drain(norms.at[0], recv_sem.at[8])
    drain(coded.at[0], recv_sem.at[7])
    decoded(partner, ROWS)
    drain(norms.at[others_far, pl.ds(0, 1)], recv_sem.at[6])
    drain(coded.at[others_far, pl.ds(0, EARLY[1])], recv_sem.at[4])

    @pl.loop(HALF + 1, N)
    def _(k):
        decoded(peer(k), EARLY[1])

    drain(rows16.at[others_far, pl.ds(0, ROWS - EARLY[1])], recv_sem.at[3])
    drain(rows16.at[others_far], recv_sem.at[9])
    drain(parts.at[:, pl.ds(0, HALF - 1)], send_sem.at[0])
    drain(sums, send_sem.at[1])
    drain(told.at[pl.ds(0, HALF - 1)], send_sem.at[2])
    drain(rows16.at[pl.ds(0, N - 1)], send_sem.at[3])
    drain(norms.at[0], send_sem.at[4])
    drain(norms.at[others_far, pl.ds(0, 1)], send_sem.at[4])
    drain(routed.at[pl.ds(0, EP - 1)], send_sem.at[5])


def store(ready, scale, router, ready_out, scale_out, router_out, sem):
    rows = ROWS // STORES
    copies = [pltpu.make_async_copy(scale, scale_out, sem.at[0]), pltpu.make_async_copy(router, router_out, sem.at[1])]
    for k in range(STORES):
        piece = pl.ds(rows * k, rows)
        copies.append(pltpu.make_async_copy(ready.at[piece], ready_out.at[piece], sem.at[2 + k]))
    for copy in copies:
        copy.start()
    for copy in copies:
        copy.wait()


def body(train_down, router_weight, router_gain):
    ready, scale, router = pl.pallas_call(
        exchange,
        out_shape=(
            jax.ShapeDtypeStruct((ROWS, N * COLS), jnp.bfloat16),
            jax.ShapeDtypeStruct((1, ROWS), jnp.float32),
            jax.ShapeDtypeStruct((EP, N * COLS), jnp.bfloat16),
        ),
        in_specs=[pl.BlockSpec(memory_space=pltpu.HBM)] * 3,
        out_specs=[pl.BlockSpec(memory_space=pltpu.VMEM)] * 3,
        scratch_shapes=[
            pltpu.VMEM((N, ROWS, COLS), jnp.float32),
            pltpu.VMEM((2, 1, COLS), jnp.float32),
            pltpu.VMEM((2, HALF, 4, 128), jnp.float32),
            pltpu.VMEM((2, HALF, 4, 128), jnp.float32),
            pltpu.VMEM((HALF, 4, 128), jnp.float32),
            pltpu.VMEM((EP, COLS), jnp.float32),
            pltpu.VMEM((16, 128), jnp.float32),
            pltpu.VMEM((16, 128), jnp.float32),
            pltpu.VMEM((24, 128), jnp.float32),
            pltpu.VMEM((HALF, 24, 128), jnp.float32),
            pltpu.VMEM((N, ROWS, COLS), jnp.bfloat16),
            pltpu.VMEM((HALF, ROWS, COLS), jnp.bfloat16),
            pltpu.SemaphoreType.DMA((N + 2,)),
            pltpu.SemaphoreType.DMA((6,)),
            pltpu.SemaphoreType.DMA((10,)),
            pltpu.SemaphoreType.REGULAR,
        ],
        compiler_params=pltpu.CompilerParams(
            collective_id=0, has_side_effects=True, vmem_limit_bytes=32 * 2**20
        ),
        name="exchange",
    )(
        *(
            pltpu.with_memory_space_constraint(array, pltpu.HBM)
            for array in (
                train_down.reshape(N, ROWS, COLS),
                router_weight.reshape(1, COLS),
                router_gain.reshape(1, COLS),
            )
        )
    )
    ready, scale, router = pl.pallas_call(
        store,
        out_shape=(
            jax.ShapeDtypeStruct(ready.shape, ready.dtype),
            jax.ShapeDtypeStruct(scale.shape, scale.dtype),
            jax.ShapeDtypeStruct(router.shape, router.dtype),
        ),
        in_specs=[pl.BlockSpec(memory_space=pltpu.VMEM)] * 3,
        out_specs=[pl.BlockSpec(memory_space=pltpu.HBM)] * 3,
        scratch_shapes=[pltpu.SemaphoreType.DMA((2 + STORES,))],
        compiler_params=pltpu.CompilerParams(vmem_limit_bytes=2**20),
        name="store",
    )(ready, scale, router)
    return ready[None], scale, router.T


def solution(mesh):
    in_specs = (P("ep", None, "fsdp"), P("fsdp", "ep"), P("fsdp"))
    out_specs = (P("ep", "fsdp", None), P("ep", "fsdp"), P())
    return jax.shard_map(body, mesh=mesh, in_specs=in_specs, out_specs=out_specs, check_vma=False)
```

```python
import jax
import jax.numpy as jnp
from jax import lax
from jax.experimental import pallas as pl
from jax.experimental.pallas import tpu as pltpu
from jax.sharding import PartitionSpec as P

MESH = pl.DeviceIdType.MESH
N = 32
EP = 8
ROWS = 448
COLS = 128
STORES = 7
HALF = N // 2
CUTS = (0, 256, 448)
EARLY = (64, 96)
POWER = 15
SPREAD = 2.0**8.4
TINY = 1e-37


def peer(k):
    f = lax.axis_index("fsdp")
    h = (f // 16 + k // 16) % 2
    y = ((f // 4) % 4 + (k // 4) % 4) % 4
    x = (f % 4 + k % 4) % 4
    return h * 16 + y * 4 + x


def send(src, dst, send_sem, recv_sem, device):
    return pltpu.make_async_remote_copy(
        src_ref=src,
        dst_ref=dst,
        send_sem=send_sem,
        recv_sem=recv_sem,
        device_id=device,
        device_id_type=MESH,
    )


def drain(ref, sem):
    pltpu.make_async_copy(ref, ref, sem).wait()


def eye():
    return lax.broadcasted_iota(jnp.int32, (128, 128), 0) == lax.broadcasted_iota(jnp.int32, (128, 128), 1)


def to_lanes(column):
    n = column.shape[0]
    return jnp.sum(jnp.where(eye()[:n], column, 0.0), axis=0, keepdims=True)


def to_column(row, start, n):
    return jnp.sum(jnp.where(eye()[start : start + n], row, 0.0), axis=1, keepdims=True)


def code(block, squares):
    u = block * (lax.rsqrt(jnp.maximum(squares, TINY)) * SPREAD)
    u2 = u * u
    u4 = u2 * u2
    return (u4 * u4 * u4 * u2 * u).astype(jnp.bfloat16)


def decode(coded, factor):
    y = coded.astype(jnp.float32)
    size = jnp.exp(jnp.log(jnp.maximum(jnp.abs(y), TINY)) * (1.0 / POWER)) * factor
    return jnp.where(y > 0.0, size, jnp.where(y < 0.0, -size, 0.0 * factor)).astype(jnp.bfloat16)


def blocks_of(first, last):
    row = first
    while row < last:
        k, start = row // 128, row % 128
        n = min(128 - start, last - row)
        yield k, start, n
        row += n


def stacked(blocks):
    return jnp.concatenate(blocks, axis=0) if len(blocks) > 1 else blocks[0]


def exchange(
    train, weight, gain, ready, scale, router,
    x, small, part, parts, norms, routed, sums, others, news, told, rows16, coded,
    load_sem, send_sem, recv_sem, far_sem,
):
    e, f = lax.axis_index("ep"), lax.axis_index("fsdp")
    half, place = f // HALF, f % HALF
    partner = peer(HALF)

    def to(device):
        return {"ep": e, "fsdp": device}

    def load(d):
        return pltpu.make_async_copy(train.at[d], x.at[d], load_sem.at[d])

    load(partner).start()
    loads = [pltpu.make_async_copy(ref, small.at[k], load_sem.at[N + k]) for k, ref in enumerate((weight, gain))]
    for copy in loads:
        copy.start()

    barrier = pltpu.get_barrier_semaphore()

    pl.semaphore_signal(barrier, inc=1, device_id=to(partner), device_id_type=MESH)

    @pl.loop(1, HALF)
    def _(k):
        pl.semaphore_signal(barrier, inc=1, device_id=to(peer(k)), device_id_type=MESH)

    @pl.loop(1, EP)
    def _(k):
        pl.semaphore_signal(barrier, inc=1, device_id={"ep": (e + k) % EP, "fsdp": f}, device_id_type=MESH)

    @pl.loop(1, N)
    def _(k):
        load(peer((HALF + k) % N)).start()

    def squares(d, coded_rows):
        load(d).wait()
        lanes = []
        for k in range(4):
            block = x[d, 128 * k : min(128 * k + 128, ROWS), :]
            column = jnp.sum(block * block, axis=1, keepdims=True)
            lanes.append(to_lanes(column))
            n = min(coded_rows - 128 * k, block.shape[0])
            if n > 0:
                rows16[d, 128 * k : 128 * k + n, :] = code(block[:n], column[:n])
        part[d // HALF, d % HALF] = jnp.concatenate(lanes, axis=0)

    squares(partner, ROWS)

    pl.semaphore_wait(barrier, HALF + EP - 1)

    pl.semaphore_signal(far_sem, inc=1, device_id=to(partner), device_id_type=MESH)
    send(part.at[partner // HALF, partner % HALF], norms.at[place], send_sem.at[4], recv_sem.at[8], to(partner)).start()
    send(rows16.at[partner], coded.at[place], send_sem.at[3], recv_sem.at[7], to(partner)).start()

    @pl.loop(HALF + 1, N)
    def _(k):
        squares(peer(k), EARLY[-1])

    @pl.loop(0, HALF)
    def _(k):
        squares(peer(k), 0)

    for copy in loads:
        copy.wait()
    mine = (small[0] * small[1]).astype(jnp.bfloat16).astype(jnp.float32)
    routed[pl.ds(e, 1), :] = mine

    @pl.loop(1, HALF)
    def _(k):
        d = peer(k)
        send(part.at[:, d % HALF], parts.at[:, place], send_sem.at[0], recv_sem.at[0], to(d)).start()

    @pl.loop(1, EP)
    def _(k):
        send(
            routed.at[pl.ds(e, 1)], routed.at[pl.ds(e, 1)], send_sem.at[5], recv_sem.at[5], {"ep": (e + k) % EP, "fsdp": f}
        ).start()

    def early(begin, end):
        rows = pl.ds(begin, end - begin)

        @pl.loop(HALF + 1, N)
        def _(k):
            d = peer(k)
            send(rows16.at[d, rows], coded.at[place, rows], send_sem.at[3], recv_sem.at[4], to(d)).start()
            if begin == 0:
                row = pl.ds(0, 1)
                send(part.at[d // HALF, d % HALF, row], norms.at[place, row], send_sem.at[4], recv_sem.at[6], to(d)).start()

    pl.semaphore_wait(far_sem, 1)
    early(0, EARLY[0])

    parts[:, place] = part[:, place]
    drain(parts.at[:, pl.ds(0, HALF - 1)], recv_sem.at[0])
    plane = jnp.sum(parts[...], axis=1)
    sums[0:4, :] = plane[0]
    sums[4:8, :] = plane[1]
    drain(routed.at[pl.ds(0, EP - 1)], recv_sem.at[5])
    sums[8:16, :] = routed[...]
    send(sums, others, send_sem.at[1], recv_sem.at[1], to(partner)).start()

    early(EARLY[0], EARLY[1])
    drain(sums, recv_sem.at[1])
    root = jnp.sqrt(sums[0:8, :] + others[0:8, :])
    news[0:8, :] = 1.0 / root
    first = half == 0
    news[8:16, :] = jnp.where(first, sums[8:16, :], others[8:16, :])
    news[16:24, :] = jnp.where(first, others[8:16, :], sums[8:16, :])

    @pl.loop(1, HALF)
    def _(k):
        send(news, told.at[place], send_sem.at[2], recv_sem.at[2], to(peer(k))).start()

    told[place] = news[...]
    own = jnp.where(first, root[0:4], root[4:8])
    for k in range(4):
        n = min(128, ROWS - 128 * k)
        scale[:, 128 * k : 128 * k + n] = own[k : k + 1, :n]

    drain(told.at[pl.ds(0, HALF - 1)], recv_sem.at[2])

    columns = pl.ds(pl.multiple_of(f * COLS, COLS), COLS)

    def ready_rows(d, first, last):
        return stacked(
            [
                (
                    x[d, 128 * k + start : 128 * k + start + n, :]
                    * to_column(told[d % HALF, pl.ds(4 * (d // HALF) + k, 1), :], start, n)
                ).astype(jnp.bfloat16)
                for k, start, n in blocks_of(first, last)
            ]
        )

    def exact(begin, end, first, last, number):
        rows = pl.ds(first, last - first)

        @pl.loop(begin, end)
        def _(k):
            d = peer(k)
            rows16[d, first:last, :] = ready_rows(d, first, last)
            send(rows16.at[d, rows], ready.at[rows, columns], send_sem.at[3], recv_sem.at[number], to(d)).start()

    for i in range(len(CUTS) - 1):
        exact(HALF + 1, N, max(CUTS[i], EARLY[1]), CUTS[i + 1], 3)
        exact(1, HALF, CUTS[i], CUTS[i + 1], 9)
    ready[:, columns] = ready_rows(f, 0, ROWS)

    for h in range(2):
        for p in range(HALF):
            at = COLS * (HALF * h + p)
            router[:, at : at + COLS] = told[p, 8 + 8 * h : 16 + 8 * h, :].astype(jnp.bfloat16)

    inverse = 1.0 / own

    def decoded(d, last):
        p = d % HALF
        at = pl.ds(pl.multiple_of(d * COLS, COLS), COLS)
        for k, start, n in blocks_of(0, last):
            factor = jnp.sqrt(jnp.maximum(norms[p, k : k + 1, :], TINY)) * inverse[k : k + 1] * (1.0 / SPREAD)
            ready[128 * k : 128 * k + n, at] = decode(coded[p, 128 * k : 128 * k + n, :], to_column(factor, start, n))

    others_far = pl.ds(0, HALF - 1)
    drain(norms.at[0], recv_sem.at[8])
    drain(coded.at[0], recv_sem.at[7])
    decoded(partner, ROWS)
    drain(norms.at[others_far, pl.ds(0, 1)], recv_sem.at[6])
    drain(coded.at[others_far, pl.ds(0, EARLY[1])], recv_sem.at[4])

    @pl.loop(HALF + 1, N)
    def _(k):
        decoded(peer(k), EARLY[1])

    drain(rows16.at[others_far, pl.ds(0, ROWS - EARLY[1])], recv_sem.at[3])
    drain(rows16.at[others_far], recv_sem.at[9])
    drain(parts.at[:, pl.ds(0, HALF - 1)], send_sem.at[0])
    drain(sums, send_sem.at[1])
    drain(told.at[pl.ds(0, HALF - 1)], send_sem.at[2])
    drain(rows16.at[pl.ds(0, N - 1)], send_sem.at[3])
    drain(norms.at[0], send_sem.at[4])
    drain(norms.at[others_far, pl.ds(0, 1)], send_sem.at[4])
    drain(routed.at[pl.ds(0, EP - 1)], send_sem.at[5])


def store(ready, scale, router, ready_out, scale_out, router_out, sem):
    rows = ROWS // STORES
    copies = [pltpu.make_async_copy(scale, scale_out, sem.at[0]), pltpu.make_async_copy(router, router_out, sem.at[1])]
    for k in range(STORES):
        piece = pl.ds(rows * k, rows)
        copies.append(pltpu.make_async_copy(ready.at[piece], ready_out.at[piece], sem.at[2 + k]))
    for copy in copies:
        copy.start()
    for copy in copies:
        copy.wait()


def body(train_down, router_weight, router_gain):
    ready, scale, router = pl.pallas_call(
        exchange,
        out_shape=(
            jax.ShapeDtypeStruct((ROWS, N * COLS), jnp.bfloat16),
            jax.ShapeDtypeStruct((1, ROWS), jnp.float32),
            jax.ShapeDtypeStruct((EP, N * COLS), jnp.bfloat16),
        ),
        in_specs=[pl.BlockSpec(memory_space=pltpu.HBM)] * 3,
        out_specs=[pl.BlockSpec(memory_space=pltpu.VMEM)] * 3,
        scratch_shapes=[
            pltpu.VMEM((N, ROWS, COLS), jnp.float32),
            pltpu.VMEM((2, 1, COLS), jnp.float32),
            pltpu.VMEM((2, HALF, 4, 128), jnp.float32),
            pltpu.VMEM((2, HALF, 4, 128), jnp.float32),
            pltpu.VMEM((HALF, 4, 128), jnp.float32),
            pltpu.VMEM((EP, COLS), jnp.float32),
            pltpu.VMEM((16, 128), jnp.float32),
            pltpu.VMEM((16, 128), jnp.float32),
            pltpu.VMEM((24, 128), jnp.float32),
            pltpu.VMEM((HALF, 24, 128), jnp.float32),
            pltpu.VMEM((N, ROWS, COLS), jnp.bfloat16),
            pltpu.VMEM((HALF, ROWS, COLS), jnp.bfloat16),
            pltpu.SemaphoreType.DMA((N + 2,)),
            pltpu.SemaphoreType.DMA((6,)),
            pltpu.SemaphoreType.DMA((10,)),
            pltpu.SemaphoreType.REGULAR,
        ],
        compiler_params=pltpu.CompilerParams(
            collective_id=0, has_side_effects=True, vmem_limit_bytes=32 * 2**20
        ),
        name="exchange",
    )(
        *(
            pltpu.with_memory_space_constraint(array, pltpu.HBM)
            for array in (
                train_down.reshape(N, ROWS, COLS),
                router_weight.reshape(1, COLS),
                router_gain.reshape(1, COLS),
            )
        )
    )
    ready, scale, router = pl.pallas_call(
        store,
        out_shape=(
            jax.ShapeDtypeStruct(ready.shape, ready.dtype),
            jax.ShapeDtypeStruct(scale.shape, scale.dtype),
            jax.ShapeDtypeStruct(router.shape, router.dtype),
        ),
        in_specs=[pl.BlockSpec(memory_space=pltpu.VMEM)] * 3,
        out_specs=[pl.BlockSpec(memory_space=pltpu.HBM)] * 3,
        scratch_shapes=[pltpu.SemaphoreType.DMA((2 + STORES,))],
        compiler_params=pltpu.CompilerParams(vmem_limit_bytes=2**20),
        name="store",
    )(ready, scale, router)
    return ready[None], scale, router.T


def solution(mesh):
    in_specs = (P("ep", None, "fsdp"), P("fsdp", "ep"), P("fsdp"))
    out_specs = (P("ep", "fsdp", None), P("ep", "fsdp"), P())
    return jax.shard_map(body, mesh=mesh, in_specs=in_specs, out_specs=out_specs, check_vma=False)
```
